32 devices in a mesh: rows: 8 (over z, x), grp: 4 (over y, core).
Axes of the slice: x: 2, y: 2, z: 4, core: 2. Of those that a mesh axis runs over, the one named last changes fastest.
Arguments:
- matrix: float32 [65536, 1024], P(('rows', 'grp'))
- row_signs: int32 [65536], P(('rows', 'grp')), may hold values from -1 to 1, as said below
- samples: int32 [8192], P(('rows', 'grp')), may hold values from 0 to 65535, as said below
Outputs:
- factor: float32 [1024, 1024], P('rows')
The draws below stay inside these ranges and needn't reach their ends.
Inputs may be any that keep to these rules, and one draw needn't show every extreme that they name: `row_signs`: every entry is 1 or -1. `samples`: entries are distinct and increasing; entries k * 256 to (k + 1) * 256 - 1 lie in rows k * 2048 to (k + 1) * 2048 - 1.
All inputs are finite; a program needn't handle non-finite values.
Results may differ from the reference program's by a relative error of at most 0.00011.
Values sent between devices are 32-bit elements; how exact they have to be, the bound alone decides.
No kernel may reach another device: no remote copies, remote signals or barrier semaphores. Data moves between devices by JAX's collectives and lax.ppermute only.
A program may use at most 128 MiB of HBM per device.

```python
import jax
import jax.numpy as jnp
from jax import lax

COLS = 1024
ROW_DEV = 2048
SAMPLES = 8192
ROWS_TOTAL = 65536


def draw_matrix(key, part):
    key_noise = jax.random.fold_in(key, 11)
    key_common = jax.random.fold_in(key, 12)
    key_cols = jax.random.fold_in(key, 13)
    col_scale = jnp.exp(jax.random.uniform(key_cols, (COLS,), jnp.float32, jnp.log(0.5), jnp.log(4.0)))
    noise = jax.random.normal(key_noise, (ROWS_TOTAL, COLS), jnp.float32)
    common = jax.random.normal(key_common, (ROWS_TOTAL, 1), jnp.float32)
    mixed_rows = noise + 0.5 * jnp.roll(noise, 1, axis=1) + 0.6 * common
    return (mixed_rows * col_scale[None, :] / jnp.sqrt(jnp.float32(ROWS_TOTAL))).astype(jnp.float32)


def draw_row_signs(key, part):
    coin_key = jax.random.fold_in(key, 21)
    return (2 * jax.random.randint(coin_key, (ROWS_TOTAL,), 0, 2) - 1).astype(jnp.int32)


def draw_samples(key, part):
    pick_key = jax.random.fold_in(key, 31)
    block_count = ROWS_TOTAL // ROW_DEV
    per_block = SAMPLES // block_count
    block_keys = jax.random.split(pick_key, block_count)
    picks = jax.vmap(lambda one_key: jnp.sort(jax.random.permutation(one_key, ROW_DEV)[:per_block]))(block_keys)
    offsets = ROW_DEV * jnp.arange(block_count, dtype=jnp.int32)[:, None]
    return (picks.astype(jnp.int32) + offsets).reshape(block_count * per_block).astype(jnp.int32)


def setup_inputs(seed: int = 0) -> dict:
    keys = jax.random.split(jax.random.key(seed), 4)
    return {
        "matrix": draw_matrix(jax.random.fold_in(keys[3], 71), 0),
        "row_signs": draw_row_signs(jax.random.fold_in(keys[3], 71), 0),
        "samples": draw_samples(jax.random.fold_in(keys[3], 71), 0),
    }


def walsh_transform(values):
    length, width_cols = values.shape
    half_span = 1
    for section_level in range(length.bit_length() - 1):
        paired = values.reshape(length // (2 * half_span), 2, half_span, width_cols)
        values = jnp.stack([paired[:, 0] + paired[:, 1], paired[:, 0] - paired[:, 1]], axis=1).reshape(length, width_cols)
        half_span = half_span * 2
    return values

def reference(matrix, row_signs, samples):
    total_rows = matrix.shape[0]
    signed = matrix * row_signs.astype(jnp.float32)[:, None]
    transformed = walsh_transform(signed) / jnp.sqrt(jnp.float32(total_rows))
    sampled = transformed[samples] * jnp.sqrt(jnp.float32(total_rows / SAMPLES))
    gram_total = jnp.dot(sampled.T, sampled, precision=lax.Precision.HIGHEST)
    lower_factor = jnp.linalg.cholesky(gram_total)
    return lower_factor.T
```

```python
import functools

import jax
import jax.numpy as jnp
from jax import lax
from jax.experimental import pallas as pl
from jax.experimental.pallas import tpu as pltpu
from jax.sharding import Mesh
from jax.sharding import PartitionSpec as P


AXES = ("hi", "mid", "grp")
LOW = ("mid", "grp")
TILE = 128
VMEM_LIMIT = 48 * 1024 * 1024


def parity(bits, length):
    shift = 1
    while shift < length.bit_length():
        shift *= 2
    while shift > 1:
        shift //= 2
        bits = bits ^ (bits >> shift)
    return bits & 1


def split2(x):
    hi = x.astype(jnp.bfloat16)
    lo = (x - hi.astype(jnp.float32)).astype(jnp.bfloat16)
    return hi, lo


def dot(a, b, dims):
    return lax.dot_general(
        a, b, dimension_numbers=(dims, ((), ())), preferred_element_type=jnp.float32
    )


def dot3(a, b, dims):
    return dot(a[0], b[0], dims) + (dot(a[0], b[1], dims) + dot(a[1], b[0], dims))


def params():
    return pltpu.CompilerParams(vmem_limit_bytes=VMEM_LIMIT)


def width_of(cols):
    return 256 if cols % 256 == 0 else TILE


def cost(flops, moved):
    return pl.CostEstimate(flops=int(flops), bytes_accessed=int(moved), transcendentals=0)


def local_kernel(signs_ref, x_ref, y_ref):
    outer, inner = signs_ref.shape
    left = lax.broadcasted_iota(jnp.int32, (inner, inner), 0)
    right = lax.broadcasted_iota(jnp.int32, (inner, inner), 1)
    hadamard = (1 - 2 * parity(left & right, inner)).astype(jnp.float32)
    parts = []
    for block in range(outer):
        signed_h = (hadamard * signs_ref[block : block + 1, :]).astype(jnp.bfloat16)
        hi, lo = split2(x_ref[block * inner : (block + 1) * inner, :])
        parts.append(dot(signed_h, hi, ((1,), (0,))) + dot(signed_h, lo, ((1,), (0,))))
    span = 1
    while span < outer:
        for start in range(outer):
            if start & span == 0:
                a, b = parts[start], parts[start + span]
                parts[start], parts[start + span] = a + b, a - b
        span *= 2
    for block in range(outer):
        y_ref[block * inner : (block + 1) * inner, :] = parts[block]


def local_transform(matrix, signs):
    rows, cols = matrix.shape
    width = width_of(cols)
    return pl.pallas_call(
        local_kernel,
        grid=(cols // width,),
        out_shape=jax.ShapeDtypeStruct((rows, cols), jnp.float32),
        in_specs=[
            pl.BlockSpec(signs.shape, lambda c: (0, 0)),
            pl.BlockSpec((rows, width), lambda c: (0, c)),
        ],
        out_specs=pl.BlockSpec((rows, width), lambda c: (0, c)),
        compiler_params=params(),
        cost_estimate=cost(4 * rows * 256 * cols, 8 * rows * cols),
    )(signs, matrix)


def pick_kernel(sel_ref, x_ref, own_ref, send_ref):
    cap = own_ref.shape[0]
    hi, lo = split2(x_ref[...])
    sel = sel_ref[...]
    out = dot(sel, hi, ((1,), (0,))) + dot(sel, lo, ((1,), (0,)))
    own_ref[...] = out[:cap]
    send_ref[...] = out[cap:]


def pick(select, arrived, first, cols):
    rows = arrived.shape[0]
    cap = select.shape[0] // 2
    width = width_of(cols)
    offset = first // width
    spec = pl.BlockSpec((cap, width), lambda c: (0, c))
    return pl.pallas_call(
        pick_kernel,
        grid=(cols // width,),
        out_shape=[jax.ShapeDtypeStruct((cap, cols), jnp.float32)] * 2,
        in_specs=[
            pl.BlockSpec(select.shape, lambda c: (0, 0)),
            pl.BlockSpec((rows, width), lambda c: (0, c + offset)),
        ],
        out_specs=[spec, spec],
        compiler_params=params(),
        cost_estimate=cost(8 * cap * rows * cols, 4 * rows * cols),
    )(select, arrived)


def packed_start(first, block):
    return sum(b + 1 for b in range(first, block))


def gram_kernel(scale, count, *refs):
    sign_ref, own_ref, got_ref = refs[:3]
    earlier, (out_ref, rows_ref) = refs[3 : 3 + count], refs[3 + count :]
    rows = (own_ref[...] * sign_ref[0:1, 0:1] + got_ref[...]) * scale
    rows_ref[...] = rows
    right = split2(rows)
    blocks = rows.shape[1] // TILE
    first = sum(ref.shape[1] for ref in earlier) // TILE
    a = 0
    for ref in [*earlier, rows_ref]:
        left = split2(ref[...])
        own = ref is rows_ref
        for part in range(ref.shape[1] // TILE):
            lanes = slice(part * TILE, (part + 1) * TILE)
            skip = part if own else 0
            piece = tuple(v[:, skip * TILE :] for v in right)
            out = dot3(tuple(v[:, lanes] for v in left), piece, ((0,), (0,)))
            for b in range(skip, blocks):
                at = (packed_start(first, first + b) + a) * TILE
                out_ref[at : at + TILE, :] = out[:, (b - skip) * TILE : (b - skip + 1) * TILE]
            a += 1


def gram(sign, own, got, earlier, scale):
    cap, cols = own.shape
    first = sum(e.shape[1] for e in earlier) // TILE
    total = packed_start(first, first + cols // TILE)
    vmem = pl.BlockSpec(memory_space=pltpu.VMEM)
    return pl.pallas_call(
        functools.partial(gram_kernel, scale, len(earlier)),
        out_shape=[
            jax.ShapeDtypeStruct((total * TILE, TILE), jnp.float32),
            jax.ShapeDtypeStruct((cap, cols), jnp.float32),
        ],
        in_specs=[vmem] * (3 + len(earlier)),
        out_specs=[vmem, vmem],
        compiler_params=params(),
        cost_estimate=cost(6 * cap * total * TILE * TILE, 8 * cap * cols),
    )(sign, own, got, *earlier)


def along_rows(x, k):
    return jnp.broadcast_to(x[k : k + 1, :], x.shape)


def along_lanes(x, k):
    return jnp.broadcast_to(x[:, k : k + 1], x.shape)


def factor_block(block, size):
    groups = size // 8
    shape = (8, size)
    rows = lax.broadcasted_iota(jnp.int32, shape, 0)
    cols = lax.broadcasted_iota(jnp.int32, shape, 1)
    upper = [block[8 * r : 8 * r + 8, :] for r in range(groups)]
    inverse = [jnp.where(cols == rows + 8 * r, 1.0, 0.0) for r in range(groups)]
    corner = [along_lanes(upper[0], c) for c in range(8)]
    for p in range(groups):
        here, more, now = 8 * p, p + 1 < groups, corner
        if more:
            left = [along_lanes(upper[p + 1], here + c) for c in range(8)]
            corner = [along_lanes(upper[p + 1], here + 8 + c) for c in range(8)]
            top = [along_lanes(upper[p], here + 8 + c) for c in range(8)]
        scale = jnp.zeros(shape, jnp.float32)
        roots, laters = [], []
        for k in range(8):
            root = lax.rsqrt(along_rows(now[k], k))
            scale = jnp.where(rows == k, root, scale)
            root = root * root
            roots.append(root)
            factor = jnp.where(rows > k, now[k] * root, 0.0)
            later = {c: along_rows(now[c], k) for c in range(k + 1, 8)}
            laters.append(later)
            upper_row, inverse_row = along_rows(upper[p], k), along_rows(inverse[p], k)
            if more:
                below = left[k] * root
                for c in range(8):
                    line = along_rows(top[c], k)
                    corner[c] = corner[c] - below * line
                    if k < 7:
                        top[c] = top[c] - factor * line
                for c in range(k + 1, 8):
                    left[c] = left[c] - below * later[c]
                upper[p + 1] = upper[p + 1] - below * upper_row
                inverse[p + 1] = inverse[p + 1] - below * inverse_row
            if k < 7:
                for c in range(k + 1, 8):
                    now[c] = now[c] - factor * later[c]
                upper[p] = upper[p] - factor * upper_row
                inverse[p] = inverse[p] - factor * inverse_row
        upper_rows = [along_rows(upper[p], k) for k in range(8)]
        inverse_rows = [along_rows(inverse[p], k) for k in range(8)]
        for r in range(p + 2, groups):
            spread = [along_lanes(upper[r], here + c) for c in range(8)]
            for k in range(8):
                below = spread[k] * roots[k]
                for c in range(k + 1, 8):
                    spread[c] = spread[c] - below * laters[k][c]
                upper[r] = upper[r] - below * upper_rows[k]
                inverse[r] = inverse[r] - below * inverse_rows[k]
        upper[p] = upper[p] * scale
        inverse[p] = inverse[p] * scale
    return upper, inverse


def factor_kernel(widths, pieces, at_ref, gram_ref, out_ref, work_ref, inverse_ref):
    cols = work_ref.shape[0]
    count = cols // TILE
    strip = TILE // pieces
    share_rows = gram_ref.shape[0] // pieces
    first = base = 0
    for width in widths:
        blocks = packed_start(first, first + width // TILE)
        for b in range(first, first + width // TILE):
            for a in range(b + 1):
                block = packed_start(first, b) + a
                for s in range(pieces):
                    line = block * TILE + s * strip
                    piece, offset = line // (blocks * strip), line % (blocks * strip)
                    at = piece * share_rows + base + offset
                    row = a * TILE + s * strip
                    work_ref[row : row + strip, b * TILE : (b + 1) * TILE] = gram_ref[
                        at : at + strip, :
                    ]
        first += width // TILE
        base += blocks * strip
    small_col = lax.broadcasted_iota(jnp.int32, (8, TILE), 1)
    small_row = lax.broadcasted_iota(jnp.int32, (8, TILE), 0)

    def step(j, carry):
        top = pl.multiple_of(j * TILE, TILE)
        here = pl.ds(top, TILE)
        upper, inverse = factor_block(work_ref[here, here], TILE)
        for r in range(TILE // 8):
            inverse_ref[8 * r : 8 * r + 8, :] = inverse[r]
            work_ref[pl.ds(top + 8 * r, 8), here] = jnp.where(
                small_col >= small_row + 8 * r, upper[r], 0.0
            )
        for block in range(count - 1):

            @pl.when(j == block)
            def _(block=block):
                rows, right = slice(block * TILE, (block + 1) * TILE), (block + 1) * TILE
                panel = dot3(
                    split2(inverse_ref[...]), split2(work_ref[rows, right:]), ((1,), (0,))
                )
                work_ref[rows, right:] = panel
                hi, lo = split2(panel)
                hi_t, lo_t = hi.T, lo.T
                for i in range(block + 1, count):
                    cut = i * TILE - right
                    lines = slice(cut, cut + TILE)
                    work_ref[i * TILE : (i + 1) * TILE, i * TILE :] -= dot3(
                        (hi_t[lines], lo_t[lines]), (hi[:, cut:], lo[:, cut:]), ((1,), (0,))
                    )

        return carry

    lax.fori_loop(0, count, step, 0)
    for i in range(1, count):
        work_ref[i * TILE : (i + 1) * TILE, : i * TILE] = jnp.zeros((TILE, i * TILE), jnp.float32)
    share = out_ref.shape[0]
    out_ref[...] = work_ref[pl.ds(pl.multiple_of(at_ref[0] * share, 8), share), :]


def factor(packed, widths, pieces, share, at):
    vmem = pl.BlockSpec(memory_space=pltpu.VMEM)
    cols = sum(widths)
    return pl.pallas_call(
        functools.partial(factor_kernel, widths, pieces),
        out_shape=jax.ShapeDtypeStruct((share, cols), jnp.float32),
        in_specs=[pl.BlockSpec(memory_space=pltpu.SMEM), vmem],
        out_specs=vmem,
        scratch_shapes=[
            pltpu.VMEM((cols, cols), jnp.float32),
            pltpu.VMEM((TILE, TILE), jnp.float32),
        ],
        compiler_params=params(),
        cost_estimate=cost(4 * cols * cols * cols, 4 * cols * cols),
    )(at, packed)


def swap(x, mask, devices):
    return lax.ppermute(x, AXES, [(i, i ^ mask) for i in range(devices)])


def bit_groups(bits):
    groups, at = [[0]], 1
    while at < bits:
        groups.append(list(range(at, min(at + 2, bits))))
        at += 2
    return groups


def arrange(parts, digit):
    count, step = len(parts), 1
    while step < count:
        flip = (digit // step) % 2 == 1
        parts = [jnp.where(flip, parts[m ^ step], parts[m]) for m in range(count)]
        step *= 2
    return jnp.concatenate(parts, axis=0)


def gather_shares(x, groups, position, devices):
    for group in groups:
        count, low = 1 << len(group), group[0]
        digit = (position >> low) & (count - 1)
        size = x.shape[0] // count
        part = [
            lax.dynamic_slice_in_dim(x, (digit ^ m) * size, size, 0) for m in range(count)
        ]
        got = [swap(part[m], m << low, devices) for m in range(1, count)]
        x = part[0]
        for g in got:
            x = x + g
    return x


def spread_shares(x, groups, position, devices):
    for group in reversed(groups):
        count, low = 1 << len(group), group[0]
        digit = (position >> low) & (count - 1)
        x = arrange([x] + [swap(x, m << low, devices) for m in range(1, count)], digit)
    return x


def select_rows(flags, cap, start):
    blocks, positions = flags.shape
    before = jnp.arange(positions)[:, None] < jnp.arange(positions)[None, :]
    within = jnp.dot(flags, before.astype(jnp.float32))
    totals = jnp.sum(flags, axis=1)
    earlier = jnp.arange(blocks)[None, :] < jnp.arange(blocks)[:, None]
    offset = jnp.sum(jnp.where(earlier, totals[None, :], 0.0), axis=1)
    rank = jnp.where(flags > 0, within + offset[:, None], -1.0).reshape(1, blocks * positions)
    wanted = (jnp.arange(cap, dtype=jnp.int32) + start).astype(jnp.float32)[:, None]
    source = jnp.arange(blocks * positions, dtype=jnp.int32)[None, :]
    found = jnp.sum(jnp.where(rank == wanted, source + 1, 0), axis=1, keepdims=True) - 1
    block, position = found // positions, found % positions
    sign = 1 - 2 * parity((source // positions) & block, blocks)
    hit = (found >= 0) & (source % positions == position)
    return jnp.where(hit, sign, 0).astype(jnp.bfloat16)


def chunk_widths(cols):
    unit = cols // 4
    if unit % TILE:
        return [cols]
    return [2 * unit, 2 * unit]


def program(matrix, row_signs, samples):
    low = lax.axis_size(LOW)
    devices = lax.axis_size(AXES)
    rows, cols = matrix.shape
    sample_dev = samples.shape[0]
    position = lax.axis_index(AXES)
    half = lax.axis_index("hi")
    owned = rows // low
    cap = -(-(5 * sample_dev) // 32) * 8
    far = devices // 2

    within = samples - position * rows
    slots = jnp.arange(rows, dtype=jnp.int32)
    flags = jnp.any(slots[:, None] == within[None, :], axis=1).astype(jnp.float32)
    flags = flags.reshape(low, owned)
    counts = jnp.broadcast_to(jnp.sum(flags, axis=1)[None, :], (low, low))
    note = jnp.concatenate([flags, counts], axis=1)
    note = lax.all_to_all(jnp.concatenate([note, note], axis=0), AXES, 0, 0, tiled=True)
    note = note.reshape(2, low, owned + low)
    most = jnp.max(jnp.sum(note[:, :, owned:], axis=1))
    rounds = (most.astype(jnp.int32) + (cap - 1)) // cap
    mine = jnp.where(half == 0, note[0], note[1])[:, :owned]
    other = jnp.where(half == 0, note[1], note[0])[:, :owned]

    def selection(start):
        return jnp.concatenate(
            [select_rows(mine, cap, start), select_rows(other, cap, start)], axis=0
        )

    inner = min(256, rows)
    signs = row_signs.astype(jnp.float32).reshape(rows // inner, inner)
    side = jnp.full((8, 128), 1 - 2 * half, jnp.int32).astype(jnp.float32)
    scale = float((sample_dev * devices) ** -0.5)
    count_rows = lax.axis_size(("hi", "mid"))
    at = lax.axis_index(("hi", "mid")).astype(jnp.int32).reshape(1)

    widths = chunk_widths(cols)
    before = local_transform(matrix, signs)
    select = selection(0)
    before, select = lax.optimization_barrier((before, select))
    arrived = lax.all_to_all(before, LOW, 0, 0, tiled=True)

    groups = bit_groups(devices.bit_length() - 1)
    first, second = groups[:2], groups[2:]
    picked, shares = [], []
    for index, width in enumerate(widths):
        own, send = pick(select, arrived, sum(widths[:index]), width)
        got = swap(send, far, devices)
        blocks, lines = gram(side, own, got, picked, scale)
        picked.append(lines)

        def more(r, total, index=index):
            again, now = selection(r * cap), []
            for i, w in enumerate(widths[: index + 1]):
                own, send = pick(again, arrived, sum(widths[:i]), w)
                total_r, lines = gram(side, own, swap(send, far, devices), now, scale)
                now.append(lines)
            return total + total_r

        blocks = lax.fori_loop(1, rounds, more, blocks)
        shares.append(gather_shares(blocks, first, position, devices))
    shared = shares[0] if len(shares) == 1 else jnp.concatenate(shares, axis=0)
    shared = gather_shares(shared, second, position, devices)
    total = spread_shares(shared, groups, position, devices)
    pieces = 1 << sum(len(g) for g in first)
    return factor(total, widths, pieces, cols // count_rows, at)


def solution(mesh):
    rows, grp = mesh.shape["rows"], mesh.shape["grp"]
    halves = Mesh(mesh.devices.reshape(2, rows // 2, grp), AXES)
    return jax.shard_map(
        program,
        mesh=halves,
        in_specs=(P(AXES, None), P(AXES), P(AXES)),
        out_specs=P(("hi", "mid"), None),
        check_vma=False,
    )
```

```python
import functools
import math

import jax
import jax.numpy as jnp
from jax import lax
from jax.experimental import pallas as pl
from jax.experimental.pallas import tpu as pltpu
from jax.sharding import Mesh
from jax.sharding import PartitionSpec as P


AXES = ("hi", "mid", "grp")
LOW = ("mid", "grp")
TILE = 128
VMEM_LIMIT = 48 * 1024 * 1024


def parity(bits, length):
    shift = 1
    while shift < length.bit_length():
        shift *= 2
    while shift > 1:
        shift //= 2
        bits = bits ^ (bits >> shift)
    return bits & 1


def split2(x):
    hi = x.astype(jnp.bfloat16)
    lo = (x - hi.astype(jnp.float32)).astype(jnp.bfloat16)
    return hi, lo


def dot(a, b, dims):
    return lax.dot_general(
        a, b, dimension_numbers=(dims, ((), ())), preferred_element_type=jnp.float32
    )


def dot3(a, b, dims):
    return dot(a[0], b[0], dims) + (dot(a[0], b[1], dims) + dot(a[1], b[0], dims))


def params():
    return pltpu.CompilerParams(vmem_limit_bytes=VMEM_LIMIT)


def width_of(cols):
    return 256 if cols % 256 == 0 else TILE


def cost(flops, moved):
    return pl.CostEstimate(flops=int(flops), bytes_accessed=int(moved), transcendentals=0)


def local_kernel(signs_ref, x_ref, y_ref):
    outer, inner = signs_ref.shape
    left = lax.broadcasted_iota(jnp.int32, (inner, inner), 0)
    right = lax.broadcasted_iota(jnp.int32, (inner, inner), 1)
    hadamard = (1 - 2 * parity(left & right, inner)).astype(jnp.float32)
    parts = []
    for block in range(outer):
        signed_h = (hadamard * signs_ref[block : block + 1, :]).astype(jnp.bfloat16)
        hi, lo = split2(x_ref[block * inner : (block + 1) * inner, :])
        parts.append(dot(signed_h, hi, ((1,), (0,))) + dot(signed_h, lo, ((1,), (0,))))
    span = 1
    while span < outer:
        for start in range(outer):
            if start & span == 0:
                a, b = parts[start], parts[start + span]
                parts[start], parts[start + span] = a + b, a - b
        span *= 2
    for block in range(outer):
        y_ref[block * inner : (block + 1) * inner, :] = parts[block]


def local_transform(matrix, signs):
    rows, cols = matrix.shape
    width = 512 if cols % 512 == 0 else width_of(cols)
    return pl.pallas_call(
        local_kernel,
        grid=(cols // width,),
        out_shape=jax.ShapeDtypeStruct((rows, cols), jnp.float32),
        in_specs=[
            pl.BlockSpec(signs.shape, lambda c: (0, 0)),
            pl.BlockSpec((rows, width), lambda c: (0, c)),
        ],
        out_specs=pl.BlockSpec((rows, width), lambda c: (0, c)),
        compiler_params=params(),
        cost_estimate=cost(4 * rows * 256 * cols, 8 * rows * cols),
    )(signs, matrix)


def pick_kernel(sel_ref, x_ref, out_ref):
    hi, lo = split2(x_ref[...])
    sel = sel_ref[...]
    out_ref[...] = dot(sel, hi, ((1,), (0,))) + dot(sel, lo, ((1,), (0,)))


def pick(select, arrived, first, cols):
    rows, cap = arrived.shape[0], select.shape[0]
    width = width_of(cols)
    offset = first // width
    return pl.pallas_call(
        pick_kernel,
        grid=(cols // width,),
        out_shape=jax.ShapeDtypeStruct((cap, cols), jnp.float32),
        in_specs=[
            pl.BlockSpec(select.shape, lambda c: (0, 0)),
            pl.BlockSpec((rows, width), lambda c: (0, c + offset)),
        ],
        out_specs=pl.BlockSpec((cap, width), lambda c: (0, c)),
        compiler_params=params(),
        cost_estimate=cost(4 * cap * rows * cols, 4 * rows * cols),
    )(select, arrived)


def select_kernel(flags_ref, out_ref):
    lists, blocks, positions = flags_ref.shape
    cap = out_ref.shape[1]
    left = lax.broadcasted_iota(jnp.int32, (positions, positions), 0)
    right = lax.broadcasted_iota(jnp.int32, (positions, positions), 1)
    before = jnp.where(left < right, 1.0, 0.0).astype(jnp.bfloat16)
    left = lax.broadcasted_iota(jnp.int32, (blocks, blocks), 0)
    right = lax.broadcasted_iota(jnp.int32, (blocks, blocks), 1)
    earlier = jnp.where(right < left, 1.0, 0.0).astype(jnp.bfloat16)
    wanted = lax.broadcasted_iota(jnp.int32, (cap, positions), 0).astype(jnp.float32)
    for n in range(lists):
        flags = flags_ref[n]
        bits = flags.astype(jnp.bfloat16)
        offset = jnp.sum(dot(earlier, bits, ((1,), (0,))), axis=1, keepdims=True)
        rank = jnp.where(flags > 0, dot(bits, before, ((1,), (0,))) + offset, -1.0)
        place = jnp.zeros((cap, positions), jnp.float32)
        block = jnp.zeros((cap, positions), jnp.float32)
        for q in range(blocks):
            hit = jnp.where(rank[q : q + 1, :] == wanted, 1.0, 0.0)
            place = place + hit
            if q:
                block = block + q * hit
        index = jnp.sum(block, axis=1, keepdims=True).astype(jnp.int32)
        parts = {0: place}
        span = 1
        while span < blocks:
            sign = jnp.where(index & span == 0, 1.0, -1.0)
            for m in range(span):
                parts[m + span] = parts[m] * sign
            span *= 2
        for m in range(blocks):
            out_ref[n, :, m * positions : (m + 1) * positions] = parts[m].astype(jnp.bfloat16)


def select_lists(mine, other, cap):
    blocks, positions = mine.shape
    if positions % TILE or cap % 16:
        return select_rows(mine, cap, 0), select_rows(other, cap, 0)
    vmem = pl.BlockSpec(memory_space=pltpu.VMEM)
    both = pl.pallas_call(
        select_kernel,
        out_shape=jax.ShapeDtypeStruct((2, cap, blocks * positions), jnp.bfloat16),
        in_specs=[vmem],
        out_specs=vmem,
        compiler_params=params(),
        cost_estimate=cost(8 * cap * blocks * positions, 4 * cap * blocks * positions),
    )(jnp.stack([mine, other]))
    return both[0], both[1]


def packed_start(first, block):
    return sum(b + 1 for b in range(first, block))


def gram_kernel(scale, count, *refs):
    sign_ref, own_ref, got_ref = refs[:3]
    earlier, (out_ref, rows_ref) = refs[3 : 3 + count], refs[3 + count :]
    rows = (own_ref[...] * sign_ref[0:1, 0:1] + got_ref[...]) * scale
    rows_ref[...] = rows
    right = split2(rows)
    blocks = rows.shape[1] // TILE
    first = sum(ref.shape[1] for ref in earlier) // TILE
    a = 0
    for ref in [*earlier, rows_ref]:
        left = split2(ref[...])
        own = ref is rows_ref
        for part in range(ref.shape[1] // TILE):
            lanes = slice(part * TILE, (part + 1) * TILE)
            skip = part if own else 0
            piece = tuple(v[:, skip * TILE :] for v in right)
            out = dot3(tuple(v[:, lanes] for v in left), piece, ((0,), (0,)))
            for b in range(skip, blocks):
                at = (packed_start(first, first + b) + a) * TILE
                out_ref[at : at + TILE, :] = out[:, (b - skip) * TILE : (b - skip + 1) * TILE]
            a += 1


def gram(sign, own, got, earlier, scale):
    cap, cols = own.shape
    first = sum(e.shape[1] for e in earlier) // TILE
    total = packed_start(first, first + cols // TILE)
    vmem = pl.BlockSpec(memory_space=pltpu.VMEM)
    return pl.pallas_call(
        functools.partial(gram_kernel, scale, len(earlier)),
        out_shape=[
            jax.ShapeDtypeStruct((total * TILE, TILE), jnp.float32),
            jax.ShapeDtypeStruct((cap, cols), jnp.float32),
        ],
        in_specs=[vmem] * (3 + len(earlier)),
        out_specs=[vmem, vmem],
        compiler_params=params(),
        cost_estimate=cost(6 * cap * total * TILE * TILE, 8 * cap * cols),
    )(sign, own, got, *earlier)


def along_rows(x, k):
    return jnp.broadcast_to(x[k : k + 1, :], x.shape)


def along_lanes(x, k):
    return jnp.broadcast_to(x[:, k : k + 1], x.shape)


def eliminate(sets, base):
    main, groups, shape = sets[0], len(sets[0]), sets[0][0].shape
    rows = lax.broadcasted_iota(jnp.int32, shape, 0)
    corner = [along_lanes(main[0], base + c) for c in range(8)]
    for p in range(groups):
        here, more, now = base + 8 * p, p + 1 < groups, corner
        if more:
            left = [along_lanes(main[p + 1], here + c) for c in range(8)]
            corner = [along_lanes(main[p + 1], here + 8 + c) for c in range(8)]
            top = [along_lanes(main[p], here + 8 + c) for c in range(8)]
        scale = jnp.zeros(shape, jnp.float32)
        roots, laters = [], []
        for k in range(8):
            root = lax.rsqrt(along_rows(now[k], k))
            scale = jnp.where(rows == k, root, scale)
            root = root * root
            roots.append(root)
            factor = jnp.where(rows > k, now[k] * root, 0.0)
            later = {c: along_rows(now[c], k) for c in range(k + 1, 8)}
            laters.append(later)
            lines = [along_rows(s[p], k) for s in sets]
            if more:
                below = left[k] * root
                for c in range(8):
                    line = along_rows(top[c], k)
                    corner[c] = corner[c] - below * line
                    if k < 7:
                        top[c] = top[c] - factor * line
                for c in range(k + 1, 8):
                    left[c] = left[c] - below * later[c]
                for s, line in zip(sets, lines):
                    s[p + 1] = s[p + 1] - below * line
            if k < 7:
                for c in range(k + 1, 8):
                    now[c] = now[c] - factor * later[c]
                for s, line in zip(sets, lines):
                    s[p] = s[p] - factor * line
        final = [[along_rows(s[p], k) for k in range(8)] for s in sets]
        for r in range(p + 2, groups):
            spread = [along_lanes(main[r], here + c) for c in range(8)]
            for k in range(8):
                below = spread[k] * roots[k]
                for c in range(k + 1, 8):
                    spread[c] = spread[c] - below * laters[k][c]
                for s, lines in zip(sets, final):
                    s[r] = s[r] - below * lines[k]
        for s in sets:
            s[p] = s[p] * scale


def rows_of(groups):
    return jnp.concatenate(groups, axis=0)


def factor_block(block):
    half = TILE // 2
    count = half // 8
    rows = lax.broadcasted_iota(jnp.int32, (8, TILE), 0)
    cols = lax.broadcasted_iota(jnp.int32, (8, TILE), 1)
    eye = [jnp.where(cols == rows + 8 * r, 1.0, 0.0) for r in range(count)]
    upper = [block[8 * r : 8 * r + 8, :] for r in range(count)]
    inverse = list(eye)
    eliminate([upper, inverse], 0)
    upper = [jnp.where(cols >= rows + 8 * r, upper[r], 0.0) for r in range(count)]
    top, inverse = rows_of(upper), rows_of(inverse)
    parts, inverse_parts = split2(top), split2(inverse)
    rest = block[half:, :] - dot3(parts, parts, ((0,), (0,)))[half:, :]
    cross = dot3(parts, inverse_parts, ((0,), (0,)))[half:, :]
    lower = [
        jnp.where(cols < half, eye[r], rest[8 * r : 8 * r + 8, :]) for r in range(count)
    ]
    eliminate([lower], half)
    corner = rows_of([jnp.where(cols >= rows + 8 * r + half, lower[r], 0.0) for r in range(count)])
    low_inverse = rows_of([jnp.where(cols < half, x, 0.0) for x in lower])
    side = dot3(split2(low_inverse[:, :half]), split2(cross), ((1,), (0,)))
    low_inverse = pltpu.roll(low_inverse, half, 1) - side
    return jnp.concatenate([top, corner], axis=0), jnp.concatenate([inverse, low_inverse], axis=0)


def stacked(a, b):
    left = jnp.concatenate([a[0], a[0], a[1]], axis=1)
    right = jnp.concatenate([b[0], b[1], b[0]], axis=0)
    return dot(left, right, ((1,), (0,)))


def unpack(gram_ref, work_ref, widths, pieces):
    strip = TILE // pieces
    share_rows = gram_ref.shape[0] // pieces
    first = base = 0
    for width in widths:
        last = first + width // TILE
        blocks = packed_start(first, last)
        for b in range(first, last):
            for a in range(b + 1):
                block = packed_start(first, b) + a
                for s in range(pieces):
                    line = block * TILE + s * strip
                    piece, offset = line // (blocks * strip), line % (blocks * strip)
                    at = piece * share_rows + base + offset
                    row = a * TILE + s * strip
                    work_ref[row : row + strip, b * TILE : (b + 1) * TILE] = gram_ref[
                        at : at + strip, :
                    ]
        first = last
        base += blocks * strip


def factor_kernel(widths, pieces, at_ref, gram_ref, out_ref, work_ref, inverse_ref):
    count = work_ref.shape[1] // TILE
    unpack(gram_ref, work_ref, widths, pieces)

    def step(j, carry):
        here = pl.ds(pl.multiple_of(j * TILE, TILE), TILE)
        upper, inverse = factor_block(work_ref[here, here])
        inverse_ref[...] = inverse
        work_ref[here, here] = upper
        for block in range(count - 1):

            @pl.when(j == block)
            def _(block=block):
                rows, right = slice(block * TILE, (block + 1) * TILE), (block + 1) * TILE
                panel = stacked(split2(inverse_ref[...]), split2(work_ref[rows, right:]))
                work_ref[rows, right:] = panel
                hi, lo = split2(panel)
                hi_t, lo_t = hi.T, lo.T
                for i in range(block + 1, count):
                    cut = i * TILE - right
                    lines = slice(cut, cut + TILE)
                    work_ref[i * TILE : (i + 1) * TILE, i * TILE :] -= stacked(
                        (hi_t[lines], lo_t[lines]), (hi[:, cut:], lo[:, cut:])
                    )

        return carry

    lax.fori_loop(0, count, step, 0)
    for i in range(1, count):
        work_ref[i * TILE : (i + 1) * TILE, : i * TILE] = jnp.zeros((TILE, i * TILE), jnp.float32)
    share = out_ref.shape[0]
    out_ref[...] = work_ref[pl.ds(pl.multiple_of(at_ref[0] * share, 8), share), :]


def factor(packed, widths, pieces, share, at):
    vmem = pl.BlockSpec(memory_space=pltpu.VMEM)
    cols = sum(widths)
    return pl.pallas_call(
        functools.partial(factor_kernel, widths, pieces),
        out_shape=jax.ShapeDtypeStruct((share, cols), jnp.float32),
        in_specs=[pl.BlockSpec(memory_space=pltpu.SMEM), vmem],
        out_specs=vmem,
        scratch_shapes=[
            pltpu.VMEM((cols, cols), jnp.float32),
            pltpu.VMEM((TILE, TILE), jnp.float32),
        ],
        compiler_params=params(),
        cost_estimate=cost(4 * cols * cols * cols, 4 * cols * cols),
    )(at, packed)


def swap(x, mask, devices):
    return lax.ppermute(x, AXES, [(i, i ^ mask) for i in range(devices)])


def bit_groups(bits):
    groups, at = [[0]], 1
    while at < bits:
        groups.append(list(range(at, min(at + 2, bits))))
        at += 2
    return groups


def arrange(parts, digit):
    count, step = len(parts), 1
    while step < count:
        flip = (digit // step) % 2 == 1
        parts = [jnp.where(flip, parts[m ^ step], parts[m]) for m in range(count)]
        step *= 2
    return jnp.concatenate(parts, axis=0)


def gather_shares(x, groups, position, devices):
    for group in groups:
        count, low = 1 << len(group), group[0]
        digit = (position >> low) & (count - 1)
        size = x.shape[0] // count
        part = [
            lax.dynamic_slice_in_dim(x, (digit ^ m) * size, size, 0) for m in range(count)
        ]
        got = [swap(part[m], m << low, devices) for m in range(1, count)]
        x = part[0]
        for g in got:
            x = x + g
    return x


def spread_shares(x, groups, position, devices):
    for group in reversed(groups):
        count, low = 1 << len(group), group[0]
        digit = (position >> low) & (count - 1)
        x = arrange([x] + [swap(x, m << low, devices) for m in range(1, count)], digit)
    return x


def select_rows(flags, cap, start):
    blocks, positions = flags.shape
    before = jnp.arange(positions)[:, None] < jnp.arange(positions)[None, :]
    within = jnp.dot(flags, before.astype(jnp.float32))
    totals = jnp.sum(flags, axis=1)
    earlier = jnp.arange(blocks)[None, :] < jnp.arange(blocks)[:, None]
    offset = jnp.sum(jnp.where(earlier, totals[None, :], 0.0), axis=1)
    rank = jnp.where(flags > 0, within + offset[:, None], -1.0).reshape(1, blocks * positions)
    wanted = (jnp.arange(cap, dtype=jnp.int32) + start).astype(jnp.float32)[:, None]
    source = jnp.arange(blocks * positions, dtype=jnp.int32)[None, :]
    found = jnp.sum(jnp.where(rank == wanted, source + 1, 0), axis=1, keepdims=True) - 1
    block, position = found // positions, found % positions
    sign = 1 - 2 * parity((source // positions) & block, blocks)
    hit = (found >= 0) & (source % positions == position)
    return jnp.where(hit, sign, 0).astype(jnp.bfloat16)


def chunk_widths(cols):
    unit = cols // 4
    if unit % TILE:
        return [cols]
    return [2 * unit, 2 * unit]


def program(matrix, row_signs, samples):
    low = lax.axis_size(LOW)
    devices = lax.axis_size(AXES)
    rows, cols = matrix.shape
    sample_dev = samples.shape[0]
    position = lax.axis_index(AXES)
    half = lax.axis_index("hi")
    owned = rows // low
    cap = -(-(sample_dev + 3 * math.isqrt(sample_dev)) // 16) * 16
    far = devices // 2

    within = samples - position * rows
    slots = jnp.arange(rows, dtype=jnp.int32)
    flags = jnp.any(slots[:, None] == within[None, :], axis=1).astype(jnp.float32)
    flags = flags.reshape(low, owned)
    counts = jnp.broadcast_to(jnp.sum(flags, axis=1)[None, :], (low, low))
    note = jnp.concatenate([flags, counts], axis=1)
    note = lax.all_to_all(jnp.concatenate([note, note], axis=0), AXES, 0, 0, tiled=True)
    note = note.reshape(2, low, owned + low)
    most = jnp.max(jnp.sum(note[:, :, owned:], axis=1))
    rounds = (most.astype(jnp.int32) + (cap - 1)) // cap
    mine = jnp.where(half == 0, note[0], note[1])[:, :owned]
    other = jnp.where(half == 0, note[1], note[0])[:, :owned]

    inner = min(256, rows)
    signs = row_signs.astype(jnp.float32).reshape(rows // inner, inner)
    scale = float((sample_dev * devices) ** -0.5)
    count_rows = lax.axis_size(("hi", "mid"))
    at = lax.axis_index(("hi", "mid")).astype(jnp.int32).reshape(1)

    widths = chunk_widths(cols)
    before = local_transform(matrix, signs)
    keep, give = select_lists(mine, other, cap)
    before, keep, give, rounds, position, half, at = lax.optimization_barrier(
        (before, keep, give, rounds, position, half, at)
    )
    arrived = lax.all_to_all(before, LOW, 0, 0, tiled=True)
    arrived, keep, give, rounds, position, half, at, mine, other = lax.optimization_barrier(
        (arrived, keep, give, rounds, position, half, at, mine, other)
    )
    side = jnp.full((8, 128), 1 - 2 * half, jnp.int32).astype(jnp.float32)

    groups = bit_groups(devices.bit_length() - 1)
    first, second = groups[:2], groups[2:]
    picked, shares, sent = [], [], []
    starts = [sum(widths[:i]) for i in range(len(widths))]
    for index, width in enumerate(widths):
        send = pick(give, arrived, starts[index], width)
        sent.append(swap(send, far, devices))
    for index, width in enumerate(widths):
        own = pick(keep, arrived, starts[index], width)
        blocks, lines = gram(side, own, sent[index], picked, scale)
        picked.append(lines)

        def more(r, total, index=index):
            now = []
            keep_r = select_rows(mine, cap, r * cap)
            give_r = select_rows(other, cap, r * cap)
            for start, w in zip(starts, widths[: index + 1]):
                got = swap(pick(give_r, arrived, start, w), far, devices)
                total_r, lines = gram(side, pick(keep_r, arrived, start, w), got, now, scale)
                now.append(lines)
            return total + total_r

        blocks = lax.fori_loop(jnp.minimum(rounds, 1), rounds, more, blocks)
        shares.append(gather_shares(blocks, first, position, devices))
    shared = shares[0] if len(shares) == 1 else jnp.concatenate(shares, axis=0)
    shared = gather_shares(shared, second, position, devices)
    total = spread_shares(shared, groups, position, devices)
    pieces = 1 << sum(len(g) for g in first)
    return factor(total, widths, pieces, cols // count_rows, at)


def solution(mesh):
    rows, grp = mesh.shape["rows"], mesh.shape["grp"]
    halves = Mesh(mesh.devices.reshape(2, rows // 2, grp), AXES)
    return jax.shard_map(
        program,
        mesh=halves,
        in_specs=(P(AXES, None), P(AXES), P(AXES)),
        out_specs=P(("hi", "mid"), None),
        check_vma=False,
    )
```

```python
import functools
import math

import jax
import jax.numpy as jnp
from jax import lax
from jax.experimental import pallas as pl
from jax.experimental.pallas import tpu as pltpu
from jax.sharding import Mesh
from jax.sharding import PartitionSpec as P


AXES = ("hi", "mid", "grp")
LOW = ("mid", "grp")
TILE = 128
VMEM_LIMIT = 48 * 1024 * 1024


def parity(bits, length):
    shift = 1
    while shift < length.bit_length():
        shift *= 2
    while shift > 1:
        shift //= 2
        bits = bits ^ (bits >> shift)
    return bits & 1


def split2(x):
    hi = x.astype(jnp.bfloat16)
    lo = (x - hi.astype(jnp.float32)).astype(jnp.bfloat16)
    return hi, lo


def dot(a, b, dims):
    return lax.dot_general(
        a, b, dimension_numbers=(dims, ((), ())), preferred_element_type=jnp.float32
    )


def dot3(a, b, dims):
    return dot(a[0], b[0], dims) + (dot(a[0], b[1], dims) + dot(a[1], b[0], dims))


def params():
    return pltpu.CompilerParams(vmem_limit_bytes=VMEM_LIMIT)


def width_of(cols):
    return 256 if cols % 256 == 0 else TILE


def cost(flops, moved):
    return pl.CostEstimate(flops=int(flops), bytes_accessed=int(moved), transcendentals=0)


def local_kernel(signs_ref, x_ref, y_ref):
    outer, inner = signs_ref.shape
    left = lax.broadcasted_iota(jnp.int32, (inner, inner), 0)
    right = lax.broadcasted_iota(jnp.int32, (inner, inner), 1)
    hadamard = (1 - 2 * parity(left & right, inner)).astype(jnp.float32)
    parts = []
    for block in range(outer):
        signed_h = (hadamard * signs_ref[block : block + 1, :]).astype(jnp.bfloat16)
        hi, lo = split2(x_ref[block * inner : (block + 1) * inner, :])
        parts.append(dot(signed_h, hi, ((1,), (0,))) + dot(signed_h, lo, ((1,), (0,))))
    span = 1
    while span < outer:
        for start in range(outer):
            if start & span == 0:
                a, b = parts[start], parts[start + span]
                parts[start], parts[start + span] = a + b, a - b
        span *= 2
    for block in range(outer):
        y_ref[block * inner : (block + 1) * inner, :] = parts[block]


def local_transform(matrix, signs):
    rows, cols = matrix.shape
    width = 512 if cols % 512 == 0 else width_of(cols)
    return pl.pallas_call(
        local_kernel,
        grid=(cols // width,),
        out_shape=jax.ShapeDtypeStruct((rows, cols), jnp.float32),
        in_specs=[
            pl.BlockSpec(signs.shape, lambda c: (0, 0)),
            pl.BlockSpec((rows, width), lambda c: (0, c)),
        ],
        out_specs=pl.BlockSpec((rows, width), lambda c: (0, c)),
        compiler_params=params(),
        cost_estimate=cost(4 * rows * 256 * cols, 8 * rows * cols),
    )(signs, matrix)


def pick_kernel(sel_ref, x_ref, out_ref):
    hi, lo = split2(x_ref[...])
    sel = sel_ref[...]
    out_ref[...] = dot(sel, hi, ((1,), (0,))) + dot(sel, lo, ((1,), (0,)))


def pick(select, arrived, first, cols):
    rows, cap = arrived.shape[0], select.shape[0]
    width = width_of(cols)
    offset = first // width
    return pl.pallas_call(
        pick_kernel,
        grid=(cols // width,),
        out_shape=jax.ShapeDtypeStruct((cap, cols), jnp.float32),
        in_specs=[
            pl.BlockSpec(select.shape, lambda c: (0, 0)),
            pl.BlockSpec((rows, width), lambda c: (0, c + offset)),
        ],
        out_specs=pl.BlockSpec((cap, width), lambda c: (0, c)),
        compiler_params=params(),
        cost_estimate=cost(4 * cap * rows * cols, 4 * rows * cols),
    )(select, arrived)


def select_kernel(flags_ref, out_ref):
    lists, blocks, positions = flags_ref.shape
    cap = out_ref.shape[1]
    left = lax.broadcasted_iota(jnp.int32, (positions, positions), 0)
    right = lax.broadcasted_iota(jnp.int32, (positions, positions), 1)
    before = jnp.where(left < right, 1.0, 0.0).astype(jnp.bfloat16)
    left = lax.broadcasted_iota(jnp.int32, (blocks, blocks), 0)
    right = lax.broadcasted_iota(jnp.int32, (blocks, blocks), 1)
    earlier = jnp.where(right < left, 1.0, 0.0).astype(jnp.bfloat16)
    wanted = lax.broadcasted_iota(jnp.int32, (cap, positions), 0).astype(jnp.float32)
    for n in range(lists):
        flags = flags_ref[n]
        bits = flags.astype(jnp.bfloat16)
        offset = jnp.sum(dot(earlier, bits, ((1,), (0,))), axis=1, keepdims=True)
        rank = jnp.where(flags > 0, dot(bits, before, ((1,), (0,))) + offset, -1.0)
        place = jnp.zeros((cap, positions), jnp.float32)
        block = jnp.zeros((cap, positions), jnp.float32)
        for q in range(blocks):
            hit = jnp.where(rank[q : q + 1, :] == wanted, 1.0, 0.0)
            place = place + hit
            if q:
                block = block + q * hit
        index = jnp.sum(block, axis=1, keepdims=True).astype(jnp.int32)
        parts = {0: place}
        span = 1
        while span < blocks:
            sign = jnp.where(index & span == 0, 1.0, -1.0)
            for m in range(span):
                parts[m + span] = parts[m] * sign
            span *= 2
        for m in range(blocks):
            out_ref[n, :, m * positions : (m + 1) * positions] = parts[m].astype(jnp.bfloat16)


def select_lists(mine, other, cap):
    blocks, positions = mine.shape
    if positions % TILE or cap % 16:
        return select_rows(mine, cap, 0), select_rows(other, cap, 0)
    vmem = pl.BlockSpec(memory_space=pltpu.VMEM)
    both = pl.pallas_call(
        select_kernel,
        out_shape=jax.ShapeDtypeStruct((2, cap, blocks * positions), jnp.bfloat16),
        in_specs=[vmem],
        out_specs=vmem,
        compiler_params=params(),
        cost_estimate=cost(8 * cap * blocks * positions, 4 * cap * blocks * positions),
    )(jnp.stack([mine, other]))
    return both[0], both[1]


def packed_start(first, block):
    return sum(b + 1 for b in range(first, block))


def gram_kernel(scale, count, *refs):
    sign_ref, own_ref, got_ref = refs[:3]
    earlier, (out_ref, rows_ref) = refs[3 : 3 + count], refs[3 + count :]
    rows = (own_ref[...] * sign_ref[0:1, 0:1] + got_ref[...]) * scale
    rows_ref[...] = rows
    hi, lo = split2(rows)
    right = jnp.concatenate([hi, lo, hi], axis=0)
    blocks = rows.shape[1] // TILE
    first = sum(ref.shape[1] for ref in earlier) // TILE
    a = 0
    for ref in [*earlier, rows_ref]:
        hi, lo = split2(ref[...])
        left = jnp.concatenate([hi, hi, lo], axis=0)
        own = ref is rows_ref
        for part in range(ref.shape[1] // TILE):
            lanes = slice(part * TILE, (part + 1) * TILE)
            skip = part if own else 0
            out = dot(left[:, lanes], right[:, skip * TILE :], ((0,), (0,)))
            for b in range(skip, blocks):
                at = (packed_start(first, first + b) + a) * TILE
                out_ref[at : at + TILE, :] = out[:, (b - skip) * TILE : (b - skip + 1) * TILE]
            a += 1


def gram(sign, own, got, earlier, scale):
    cap, cols = own.shape
    first = sum(e.shape[1] for e in earlier) // TILE
    total = packed_start(first, first + cols // TILE)
    vmem = pl.BlockSpec(memory_space=pltpu.VMEM)
    return pl.pallas_call(
        functools.partial(gram_kernel, scale, len(earlier)),
        out_shape=[
            jax.ShapeDtypeStruct((total * TILE, TILE), jnp.float32),
            jax.ShapeDtypeStruct((cap, cols), jnp.float32),
        ],
        in_specs=[vmem] * (3 + len(earlier)),
        out_specs=[vmem, vmem],
        compiler_params=params(),
        cost_estimate=cost(6 * cap * total * TILE * TILE, 8 * cap * cols),
    )(sign, own, got, *earlier)


def along_rows(x, k):
    return jnp.broadcast_to(x[k : k + 1, :], x.shape)


def along_lanes(x, k):
    return jnp.broadcast_to(x[:, k : k + 1], x.shape)


def eliminate(sets, base):
    main, groups, shape = sets[0], len(sets[0]), sets[0][0].shape
    rows = lax.broadcasted_iota(jnp.int32, shape, 0)
    corner = [along_lanes(main[0], base + c) for c in range(8)]
    for p in range(groups):
        here, more, now = base + 8 * p, p + 1 < groups, corner
        if more:
            left = [along_lanes(main[p + 1], here + c) for c in range(8)]
            corner = [along_lanes(main[p + 1], here + 8 + c) for c in range(8)]
            top = [along_lanes(main[p], here + 8 + c) for c in range(8)]
        scale = jnp.zeros(shape, jnp.float32)
        roots, laters = [], []
        for k in range(8):
            root = lax.rsqrt(along_rows(now[k], k))
            scale = jnp.where(rows == k, root, scale)
            root = root * root
            roots.append(root)
            factor = jnp.where(rows > k, now[k] * root, 0.0)
            later = {c: along_rows(now[c], k) for c in range(k + 1, 8)}
            laters.append(later)
            lines = [along_rows(s[p], k) for s in sets]
            if more:
                below = left[k] * root
                for c in range(8):
                    line = along_rows(top[c], k)
                    corner[c] = corner[c] - below * line
                    if k < 7:
                        top[c] = top[c] - factor * line
                for c in range(k + 1, 8):
                    left[c] = left[c] - below * later[c]
                for s, line in zip(sets, lines):
                    s[p + 1] = s[p + 1] - below * line
            if k < 7:
                for c in range(k + 1, 8):
                    now[c] = now[c] - factor * later[c]
                for s, line in zip(sets, lines):
                    s[p] = s[p] - factor * line
        final = [[along_rows(s[p], k) for k in range(8)] for s in sets]
        for r in range(p + 2, groups):
            spread = [along_lanes(main[r], here + c) for c in range(8)]
            for k in range(8):
                below = spread[k] * roots[k]
                for c in range(k + 1, 8):
                    spread[c] = spread[c] - below * laters[k][c]
                for s, lines in zip(sets, final):
                    s[r] = s[r] - below * lines[k]
        for s in sets:
            s[p] = s[p] * scale


def rows_of(groups):
    return jnp.concatenate(groups, axis=0)


def factor_block(block):
    half = TILE // 2
    count = half // 8
    rows = lax.broadcasted_iota(jnp.int32, (8, TILE), 0)
    cols = lax.broadcasted_iota(jnp.int32, (8, TILE), 1)
    eye = [jnp.where(cols == rows + 8 * r, 1.0, 0.0) for r in range(count)]
    upper = [block[8 * r : 8 * r + 8, :] for r in range(count)]
    inverse = list(eye)
    eliminate([upper, inverse], 0)
    upper = [jnp.where(cols >= rows + 8 * r, upper[r], 0.0) for r in range(count)]
    top, inverse = rows_of(upper), rows_of(inverse)
    parts, inverse_parts = split2(top), split2(inverse)
    rest = block[half:, :] - dot3(parts, parts, ((0,), (0,)))[half:, :]
    cross = dot3(parts, inverse_parts, ((0,), (0,)))[half:, :]
    lower = [
        jnp.where(cols < half, eye[r], rest[8 * r : 8 * r + 8, :]) for r in range(count)
    ]
    eliminate([lower], half)
    corner = rows_of([jnp.where(cols >= rows + 8 * r + half, lower[r], 0.0) for r in range(count)])
    low_inverse = rows_of([jnp.where(cols < half, x, 0.0) for x in lower])
    side = dot3(split2(low_inverse[:, :half]), split2(cross), ((1,), (0,)))
    low_inverse = pltpu.roll(low_inverse, half, 1) - side
    return jnp.concatenate([top, corner], axis=0), jnp.concatenate([inverse, low_inverse], axis=0)


def stacked(a, b):
    left = jnp.concatenate([a[0], a[0], a[1]], axis=1)
    right = jnp.concatenate([b[0], b[1], b[0]], axis=0)
    return dot(left, right, ((1,), (0,)))


def unpack(gram_ref, work_ref, widths, pieces):
    strip = TILE // pieces
    share_rows = gram_ref.shape[0] // pieces
    first = base = 0
    for width in widths:
        last = first + width // TILE
        blocks = packed_start(first, last)
        for b in range(first, last):
            for a in range(b + 1):
                block = packed_start(first, b) + a
                for s in range(pieces):
                    line = block * TILE + s * strip
                    piece, offset = line // (blocks * strip), line % (blocks * strip)
                    at = piece * share_rows + base + offset
                    row = a * TILE + s * strip
                    work_ref[row : row + strip, b * TILE : (b + 1) * TILE] = gram_ref[
                        at : at + strip, :
                    ]
        first = last
        base += blocks * strip


def factor_kernel(widths, pieces, at_ref, gram_ref, out_ref, work_ref, inverse_ref):
    count = work_ref.shape[1] // TILE
    unpack(gram_ref, work_ref, widths, pieces)

    def step(j, carry):
        here = pl.ds(pl.multiple_of(j * TILE, TILE), TILE)
        upper, inverse = factor_block(work_ref[here, here])
        inverse_ref[...] = inverse
        work_ref[here, here] = upper
        for block in range(count - 1):

            @pl.when(j == block)
            def _(block=block):
                rows, right = slice(block * TILE, (block + 1) * TILE), (block + 1) * TILE
                panel = stacked(split2(inverse_ref[...]), split2(work_ref[rows, right:]))
                work_ref[rows, right:] = panel
                hi, lo = split2(panel)
                hi_t, lo_t = hi.T, lo.T
                for i in range(block + 1, count):
                    cut = i * TILE - right
                    lines = slice(cut, cut + TILE)
                    work_ref[i * TILE : (i + 1) * TILE, i * TILE :] -= stacked(
                        (hi_t[lines], lo_t[lines]), (hi[:, cut:], lo[:, cut:])
                    )

        return carry

    lax.fori_loop(0, count, step, 0)
    for i in range(1, count):
        work_ref[i * TILE : (i + 1) * TILE, : i * TILE] = jnp.zeros((TILE, i * TILE), jnp.float32)
    share = out_ref.shape[0]
    out_ref[...] = work_ref[pl.ds(pl.multiple_of(at_ref[0] * share, 8), share), :]


def factor(packed, widths, pieces, share, at):
    vmem = pl.BlockSpec(memory_space=pltpu.VMEM)
    cols = sum(widths)
    return pl.pallas_call(
        functools.partial(factor_kernel, widths, pieces),
        out_shape=jax.ShapeDtypeStruct((share, cols), jnp.float32),
        in_specs=[pl.BlockSpec(memory_space=pltpu.SMEM), vmem],
        out_specs=vmem,
        scratch_shapes=[
            pltpu.VMEM((cols, cols), jnp.float32),
            pltpu.VMEM((TILE, TILE), jnp.float32),
        ],
        compiler_params=params(),
        cost_estimate=cost(4 * cols * cols * cols, 4 * cols * cols),
    )(at, packed)


def swap(x, mask, devices):
    return lax.ppermute(x, AXES, [(i, i ^ mask) for i in range(devices)])


def bit_groups(bits):
    groups, at = [[0]], 1
    while at < bits:
        groups.append(list(range(at, min(at + 2, bits))))
        at += 2
    return groups


def arrange(parts, digit):
    count, step = len(parts), 1
    while step < count:
        flip = (digit // step) % 2 == 1
        parts = [jnp.where(flip, parts[m ^ step], parts[m]) for m in range(count)]
        step *= 2
    return jnp.concatenate(parts, axis=0)


def gather_shares(x, groups, position, devices):
    for group in groups:
        count, low = 1 << len(group), group[0]
        digit = (position >> low) & (count - 1)
        size = x.shape[0] // count
        part = [
            lax.dynamic_slice_in_dim(x, (digit ^ m) * size, size, 0) for m in range(count)
        ]
        got = [swap(part[m], m << low, devices) for m in range(1, count)]
        x = part[0]
        for g in got:
            x = x + g
    return x


def spread_shares(x, groups, position, devices):
    for group in reversed(groups):
        count, low = 1 << len(group), group[0]
        digit = (position >> low) & (count - 1)
        x = arrange([x] + [swap(x, m << low, devices) for m in range(1, count)], digit)
    return x


def select_rows(flags, cap, start):
    blocks, positions = flags.shape
    before = jnp.arange(positions)[:, None] < jnp.arange(positions)[None, :]
    within = jnp.dot(flags, before.astype(jnp.float32))
    totals = jnp.sum(flags, axis=1)
    earlier = jnp.arange(blocks)[None, :] < jnp.arange(blocks)[:, None]
    offset = jnp.sum(jnp.where(earlier, totals[None, :], 0.0), axis=1)
    rank = jnp.where(flags > 0, within + offset[:, None], -1.0).reshape(1, blocks * positions)
    wanted = (jnp.arange(cap, dtype=jnp.int32) + start).astype(jnp.float32)[:, None]
    source = jnp.arange(blocks * positions, dtype=jnp.int32)[None, :]
    found = jnp.sum(jnp.where(rank == wanted, source + 1, 0), axis=1, keepdims=True) - 1
    block, position = found // positions, found % positions
    sign = 1 - 2 * parity((source // positions) & block, blocks)
    hit = (found >= 0) & (source % positions == position)
    return jnp.where(hit, sign, 0).astype(jnp.bfloat16)


def chunk_widths(cols):
    unit = cols // 4
    if unit % TILE:
        return [cols]
    return [2 * unit, 2 * unit]


def program(matrix, row_signs, samples):
    low = lax.axis_size(LOW)
    devices = lax.axis_size(AXES)
    rows, cols = matrix.shape
    sample_dev = samples.shape[0]
    position = lax.axis_index(AXES)
    half = lax.axis_index("hi")
    owned = rows // low
    cap = -(-(sample_dev + 3 * math.isqrt(sample_dev)) // 16) * 16
    far = devices // 2

    within = samples - position * rows
    slots = jnp.arange(rows, dtype=jnp.int32)
    flags = jnp.any(slots[:, None] == within[None, :], axis=1).astype(jnp.float32)
    flags = flags.reshape(low, owned)
    counts = jnp.broadcast_to(jnp.sum(flags, axis=1)[None, :], (low, low))
    note = jnp.concatenate([flags, counts], axis=1)
    note = lax.all_to_all(jnp.concatenate([note, note], axis=0), AXES, 0, 0, tiled=True)
    note = note.reshape(2, low, owned + low)
    most = jnp.max(jnp.sum(note[:, :, owned:], axis=1))
    rounds = (most.astype(jnp.int32) + (cap - 1)) // cap
    mine = jnp.where(half == 0, note[0], note[1])[:, :owned]
    other = jnp.where(half == 0, note[1], note[0])[:, :owned]

    inner = min(256, rows)
    signs = row_signs.astype(jnp.float32).reshape(rows // inner, inner)
    scale = float((sample_dev * devices) ** -0.5)
    count_rows = lax.axis_size(("hi", "mid"))
    at = lax.axis_index(("hi", "mid")).astype(jnp.int32).reshape(1)

    widths = chunk_widths(cols)
    before = local_transform(matrix, signs)
    keep, give = select_lists(mine, other, cap)
    before, keep, give, rounds, position, half, at = lax.optimization_barrier(
        (before, keep, give, rounds, position, half, at)
    )
    arrived = lax.all_to_all(before, LOW, 0, 0, tiled=True)
    arrived, keep, give, rounds, position, half, at, mine, other = lax.optimization_barrier(
        (arrived, keep, give, rounds, position, half, at, mine, other)
    )
    side = jnp.full((8, 128), 1 - 2 * half, jnp.int32).astype(jnp.float32)

    groups = bit_groups(devices.bit_length() - 1)
    first, second = groups[:2], groups[2:]
    picked, shares, sent = [], [], []
    starts = [sum(widths[:i]) for i in range(len(widths))]
    for index, width in enumerate(widths):
        send = pick(give, arrived, starts[index], width)
        sent.append(swap(send, far, devices))
    for index, width in enumerate(widths):
        own = pick(keep, arrived, starts[index], width)
        blocks, lines = gram(side, own, sent[index], picked, scale)
        picked.append(lines)

        def more(r, total, index=index):
            now = []
            keep_r = select_rows(mine, cap, r * cap)
            give_r = select_rows(other, cap, r * cap)
            for start, w in zip(starts, widths[: index + 1]):
                got = swap(pick(give_r, arrived, start, w), far, devices)
                total_r, lines = gram(side, pick(keep_r, arrived, start, w), got, now, scale)
                now.append(lines)
            return total + total_r

        blocks = lax.fori_loop(jnp.minimum(rounds, 1), rounds, more, blocks)
        shares.append(gather_shares(blocks, first, position, devices))
    shared = shares[0] if len(shares) == 1 else jnp.concatenate(shares, axis=0)
    shared = gather_shares(shared, second, position, devices)
    total = spread_shares(shared, groups, position, devices)
    pieces = 1 << sum(len(g) for g in first)
    return factor(total, widths, pieces, cols // count_rows, at)


def solution(mesh):
    rows, grp = mesh.shape["rows"], mesh.shape["grp"]
    halves = Mesh(mesh.devices.reshape(2, rows // 2, grp), AXES)
    return jax.shard_map(
        program,
        mesh=halves,
        in_specs=(P(AXES, None), P(AXES), P(AXES)),
        out_specs=P(("hi", "mid"), None),
        check_vma=False,
    )
```
